512 devices in a mesh: group: 2 (over y), slab: 16 (over z), subj: 8 (over x), yslab: 2 (over core).
Axes of the slice: x: 8, y: 2, z: 16, core: 2. Of those that a mesh axis runs over, the one named last changes fastest.
The devices are a block of a 8x16x16 slice.
Arguments:
- subjects: bfloat16 [16, 256, 16, 256], P(('group', 'subj'), 'slab', 'yslab'), parts along dimension 0, may hold values from -6 to 6
- offsets: int32 [16, 3, 256, 16, 256], P(('group', 'subj'), None, 'slab', 'yslab'), parts along dimension 0, may hold values from -2 to 1
- template: float32 [512, 16, 256], P(('group', 'slab'), 'yslab'), parts along dimension 0, may hold values from -6 to 6
- control: float32 [16, 3, 67, 7, 128], P(('group', 'subj')), parts along dimension 0, may hold values from -8 to 8
Outputs:
- template_out: float32 [512, 16, 256], P(('group', 'slab'), 'yslab'), parts along dimension 0
- control_out: float32 [16, 3, 67, 7, 128], P(('group', 'subj')), parts along dimension 0
The draws below stay inside these ranges and needn't reach their ends.
There are 2 independent parts, one for each index of `group`. The reference program is written for one: setup_inputs(seed, part) draws one part's arguments, and reference() takes and returns one part's arrays. A program takes and returns all parts, laid end to end along the dimension named above; each array names one. Nothing has to cross between parts.
All inputs are finite; a program needn't handle non-finite values.
Results may differ from the reference program's by a relative error of at most 0.00065.
Values may be sent and summed in bfloat16 or wider, within the bound.
A program may use at most 64 MiB of HBM per device.

```python
import jax
import jax.numpy as jnp
from jax import lax

NX = 256
KNOT = 4
KNOT_X = 2
HALO = 2
ITERS = 2
NZ = 256
NY = 16
NS = 8
GZ = 67
GY = 7
GX = 128


def plant(array, own_key, least, top_value):
    longest = array.shape.index(max(array.shape))
    spots = []
    for shift in (0, 1):
        where = [jax.random.randint(jax.random.fold_in(own_key, axis), (), 0, length) for axis, length in enumerate(array.shape)]
        where[longest] = (where[longest] + shift) % array.shape[longest]
        spots.append(tuple(where))
    return array.at[spots[0]].set(least).at[spots[1]].set(top_value)


def shard_levels(stream_key, extent, shards, smallest, top_value):
    def one(position, shards_of):
        heights = jax.random.uniform(jax.random.fold_in(jax.random.fold_in(stream_key, 6), position), (shards_of,), jnp.float32, smallest / len(shards), top_value / len(shards))
        return jnp.repeat(jnp.exp(heights), extent[position] // shards_of).reshape((-1,) + (1,) * (len(extent) - position - 1))

    level = one(*shards[0])
    for cut in shards[1:]:
        level = level * one(*cut)
    return level


def bell_draw(stream_key, extent, scale, reach, shards=(), kind=jnp.bfloat16):
    values = jax.random.normal(stream_key, extent, jnp.float32) * scale
    if len(shards) > 0:
        values = shard_levels(stream_key, extent, shards, -0.22, 0.18) * values
    return jnp.clip(values, min=-reach, max=reach).astype(kind)


def setup_inputs(seed: int = 0, part: int = 0) -> dict:
    seeds = jax.random.split(jax.random.key(seed), 5)
    part_keys = jax.random.split(jax.random.fold_in(seeds[4], part), 5)
    return {
        "subjects": bell_draw(part_keys[0], (NS, NZ, NY, NX), 1.0, 6.0, ((0, 8), (1, 16), (2, 2))),
        "offsets": plant(jax.random.randint(part_keys[1], (NS, 3, NZ, NY, NX), -HALO, HALO), jax.random.fold_in(part_keys[1], 1), -HALO, HALO - 1).astype(jnp.int32),
        "template": bell_draw(part_keys[2], (NZ, NY, NX), 1.0, 6.0, ((0, 16), (1, 2)), jnp.float32),
        "control": bell_draw(part_keys[3], (NS, 3, GZ, GY, GX), 2.0, 8.0, ((0, 8),), jnp.float32),
    }


step_length = 0.5
tiny_term = 1e-06

def basis(positions, columns, spacing, wrap):
    cell = positions // spacing
    frac = (positions - cell * spacing).astype(jnp.float32) / spacing
    weights = [(1.0 - frac) ** 3 / 6.0, (3.0 * frac ** 3 - 6.0 * frac ** 2 + 4.0) / 6.0, (-3.0 * frac ** 3 + 3.0 * frac ** 2 + 3.0 * frac + 1.0) / 6.0, frac ** 3 / 6.0]
    index = jnp.arange(columns, dtype=jnp.int32)
    matrix = jnp.zeros((positions.shape[0], columns), jnp.float32)
    for offset in range(4):
        target = cell + offset
        if wrap:
            target = target % columns
        matrix = matrix + jnp.where(index[None, :] == target[:, None], weights[offset][:, None], 0.0)
    return matrix

def forward_field(coeffs, basis_z, basis_y, basis_x):
    high = lax.Precision.HIGHEST
    first = jnp.einsum('cabg,za->czbg', coeffs, basis_z, precision=high)
    second = jnp.einsum('czbg,yb->czyg', first, basis_y, precision=high)
    return jnp.einsum('czyg,xg->czyx', second, basis_x, precision=high)

def adjoint_field(gradient, basis_z, basis_y, basis_x):
    high = lax.Precision.HIGHEST
    first = jnp.einsum('czyx,xg->czyg', gradient, basis_x, precision=high)
    second = jnp.einsum('czyg,yb->czbg', first, basis_y, precision=high)
    return jnp.einsum('czbg,za->cabg', second, basis_z, precision=high)

def trilinear(flat, base_z, base_y, base_x, size_y, size_x, fraction):

    def corner_value(step_z, step_y, step_x):
        index = ((base_z + step_z) * size_y + base_y + step_y) * size_x + base_x + step_x
        return jnp.take(flat, index).astype(jnp.float32)
    frac_z, frac_y, frac_x = (fraction[0], fraction[1], fraction[2])
    along_x = {}
    diff_x = {}
    for step_z in range(2):
        for step_y in range(2):
            low = corner_value(step_z, step_y, 0)
            high = corner_value(step_z, step_y, 1)
            along_x[step_z, step_y] = low * (1.0 - frac_x) + high * frac_x
            diff_x[step_z, step_y] = high - low
    along_y = []
    diff_y = []
    diff_xy = []
    for step_z in range(2):
        along_y.append(along_x[step_z, 0] * (1.0 - frac_y) + along_x[step_z, 1] * frac_y)
        diff_y.append(along_x[step_z, 1] - along_x[step_z, 0])
        diff_xy.append(diff_x[step_z, 0] * (1.0 - frac_y) + diff_x[step_z, 1] * frac_y)
    warped = along_y[0] * (1.0 - frac_z) + along_y[1] * frac_z
    slope_z = along_y[1] - along_y[0]
    slope_y = diff_y[0] * (1.0 - frac_z) + diff_y[1] * frac_z
    slope_x = diff_xy[0] * (1.0 - frac_z) + diff_xy[1] * frac_z
    return (warped, jnp.stack([slope_z, slope_y, slope_x]))

def reference(subjects, offsets, template, control):
    depth, height, width = (subjects.shape[1], subjects.shape[2], subjects.shape[3])
    basis_z = basis(jnp.arange(depth, dtype=jnp.int32), control.shape[2], KNOT, False)
    basis_y = basis(jnp.arange(height, dtype=jnp.int32), control.shape[3], KNOT, False)
    basis_x = basis(jnp.arange(width, dtype=jnp.int32), control.shape[4], KNOT_X, True)
    coord_z = jnp.arange(depth, dtype=jnp.int32)[:, None, None] + HALO
    coord_y = jnp.arange(height, dtype=jnp.int32)[None, :, None] + HALO
    coord_x = jnp.arange(width, dtype=jnp.int32)[None, None, :] + HALO
    size_y = height + 2 * HALO
    size_x = width + 2 * HALO
    current = template
    coeffs_all = control
    for iteration in range(ITERS):

        def per_subject(total, item):
            volume, shifts, coeffs = item
            padded = jnp.pad(volume, HALO).reshape(-1)
            displace = forward_field(coeffs, basis_z, basis_y, basis_x)
            tanh_u = jnp.tanh(displace)
            fraction = 0.5 + 0.5 * tanh_u
            warped, slopes = trilinear(padded, coord_z + shifts[0], coord_y + shifts[1], coord_x + shifts[2], size_y, size_x, fraction)
            resid = warped - current
            grad_u = resid[None] * slopes * (1.0 - tanh_u * tanh_u)
            grid = adjoint_field(grad_u, basis_z, basis_y, basis_x)
            peak = jnp.max(jnp.sqrt(lax.optimization_barrier(jnp.sum(grid * grid, axis=0))))
            updated = coeffs - step_length * grid / (peak + tiny_term)
            return (total + warped, updated)
        total, coeffs_all = lax.scan(per_subject, jnp.zeros(current.shape, jnp.float32), (subjects, offsets, coeffs_all))
        current = total / subjects.shape[0]
    return (current, coeffs_all)
```

```python
import jax
import jax.numpy as jnp
import numpy as np
from jax import lax
from jax.experimental import pallas as pl
from jax.experimental.pallas import tpu as pltpu
from jax.sharding import PartitionSpec as P

KNOT = 4
HALO = 2
STEP = 0.5
TINY = 1e-06
CUBE = 384.0
CUBE_X = 48.0
SCALE = 1.0 / (CUBE * CUBE * CUBE_X)
F32 = jnp.float32
BF16 = jnp.bfloat16
MESH = pl.DeviceIdType.MESH


def spline(count, columns, spacing, wrap):
    whole = 6 * spacing**3
    matrix = np.zeros((count, columns))
    for t in range(count):
        j = t // spacing
        s = (t - j * spacing) / spacing
        weights = [
            (1 - s) ** 3 / 6,
            (3 * s**3 - 6 * s**2 + 4) / 6,
            (-3 * s**3 + 3 * s**2 + 3 * s + 1) / 6,
            s**3 / 6,
        ]
        for o in range(4):
            column = (j + o) % columns if wrap else j + o
            matrix[t, column] += weights[o] * whole
    return np.rint(matrix)


def halves(whole):
    high = np.asarray(whole, np.float32).astype(BF16).astype(np.float32)
    low = (whole - high).astype(np.float32)
    assert (low.astype(BF16).astype(np.float32) == low).all()
    return high, low


def constants(depth, height, width, columns_x):
    assert (depth, height) == (16, 8)
    bz = spline(depth, 7, KNOT, False)
    by = spline(height, 5, KNOT, False)
    forward = np.zeros((2, depth, height, 8, 8))
    for k in range(2):
        forward[k, :, :, :7, 2 * k : 2 * k + 5] = np.einsum("za,yb->zyab", bz, by)
    forward = forward.reshape(2, depth * height, 64)
    high, low = halves(forward)
    forward = np.concatenate([high, low, high], axis=2)
    adjoint = np.zeros((3, 16, depth, height))
    for group, rows in enumerate(([0, 1, 2], [4, 5, 6], [3])):
        for place, a in enumerate(rows):
            for b in range(5):
                adjoint[group, place * 5 + b] = np.outer(bz[:, a], by[:, b])
    adjoint = adjoint.reshape(48, depth * height)
    high, low = halves(adjoint)
    adjoint = np.concatenate([high, low, high], axis=1)
    gather = np.zeros((3, 64, 10, 16))
    for edge in range(3):
        for a in range(7):
            for b in range(7):
                for k in range(2):
                    c = b - 2 * k
                    if not 0 <= c < 5:
                        continue
                    row = a * 8 + b
                    if a < 3:
                        gather[edge, row, 3 * k, a * 5 + c] = 1
                        if edge != 1:
                            gather[edge, row, 6 + k, a * 5 + c] = 1
                    elif a == 3:
                        gather[edge, row, 3 * k + 2, c] = 1
                    else:
                        gather[edge, row, 3 * k + 1, (a - 4) * 5 + c] = 1
                        if edge != 2:
                            gather[edge, row, 8 + k, (a - 4) * 5 + c] = 1
    gather = gather.reshape(3, 64, 160)
    bx = spline(width, columns_x, 2, True)
    across = np.concatenate([bx.T, bx.T], axis=0)
    return [jnp.asarray(m, BF16) for m in (forward, across, bx, adjoint, gather)]


def split(x):
    high = x.astype(BF16)
    return high, (x - high.astype(F32)).astype(BF16)


def dot(a, b):
    return jnp.dot(a, b, preferred_element_type=F32)


def field(coeffs, wf, bxt, out):
    for c in range(3):
        high, low = split(coeffs[c])
        first = dot(wf, jnp.concatenate([high, high, low], axis=0))
        high, low = split(first)
        out[c] = dot(jnp.concatenate([high, low], axis=1), bxt) * SCALE


def send(src, dst, send_sem, recv_sem, **where):
    return pltpu.make_async_remote_copy(
        src_ref=src,
        dst_ref=dst,
        send_sem=send_sem,
        recv_sem=recv_sem,
        device_id=where,
        device_id_type=MESH,
    )


def greet(barrier, **where):
    pl.semaphore_signal(barrier, inc=1, device_id=where, device_id_type=MESH)


def each(first, last, body):
    def step(i, carry):
        body(i)
        return carry

    lax.fori_loop(first, last, step, 0)


def halo_kernel(
    slabs, subject, control, wf, bxt, own_out, peer_out, u_out,
    own, peer, band, coeffs, band_sem, send_sem, recv_sem,
):
    me = lax.axis_index("slab")
    core = lax.axis_index("yslab")
    depth = subject.shape[0]
    up = lax.rem(me + 1, slabs)
    down = lax.rem(me + slabs - 1, slabs)
    other = 1 - core
    barrier = pltpu.get_barrier_semaphore()
    greet(barrier, yslab=other)
    for slab in (up, down):
        greet(barrier, slab=slab)
        greet(barrier, slab=slab, yslab=other)
    fetch = pltpu.make_async_copy(control.at[:, pl.ds(me * (depth // KNOT), 7)], band, band_sem)
    fetch.start()
    coeffs[...] = jnp.zeros_like(coeffs)
    pl.semaphore_wait(barrier, 5)
    inner = pl.ds(HALO, depth)
    low = pl.ds(0, HALO)
    high = pl.ds(depth + HALO, HALO)
    first = pl.ds(0, HALO)
    last = pl.ds(depth - HALO, HALO)
    plan = [
        (subject, peer.at[inner], dict(yslab=other)),
        (subject.at[last], own.at[low], dict(slab=up)),
        (subject.at[last], peer.at[low], dict(slab=up, yslab=other)),
        (subject.at[first], own.at[high], dict(slab=down)),
        (subject.at[first], peer.at[high], dict(slab=down, yslab=other)),
    ]
    copies = [
        send(src, dst, send_sem.at[i], recv_sem.at[i], **where)
        for i, (src, dst, where) in enumerate(plan)
    ]
    for copy in copies[1:] + copies[:1]:
        copy.start()
    own_out[HALO : HALO + depth] = subject[...]
    fetch.wait()
    for c in range(3):
        coeffs[c, 0:7, 0:7, :] = band[c]
    field([coeffs[c].reshape(64, 128) for c in range(3)], wf[core], bxt[...], u_out)
    for copy in copies:
        copy.wait()
    own_out[0:HALO] = own[0:HALO]
    own_out[HALO + depth :] = own[HALO + depth :]
    peer_out[...] = peer[...]


def pick(shift, values):
    odd, top = shift
    steps = [jnp.where(odd, values[i + 1], values[i]) for i in range(4)]
    return jnp.where(top, steps[2], steps[0]), jnp.where(top, steps[3], steps[1])


def pick_many(shift, groups):
    pairs = [pick(shift, values) for values in zip(*groups)]
    return [p[0] for p in pairs], [p[1] for p in pairs]


def warp(lows, steps, u, current):
    th = [jnp.tanh(x) for x in u]
    fz, fy, fx = [0.5 + 0.5 * t for t in th]
    along = [low + fx * step for low, step in zip(lows, steps)]
    slope_y = [along[1] - along[0], along[3] - along[2]]
    along_y = [along[0] + fy * slope_y[0], along[2] + fy * slope_y[1]]
    slope_x = [steps[0] + fy * (steps[1] - steps[0]), steps[2] + fy * (steps[3] - steps[2])]
    slopes = [
        along_y[1] - along_y[0],
        slope_y[0] + fz * (slope_y[1] - slope_y[0]),
        slope_x[0] + fz * (slope_x[1] - slope_x[0]),
    ]
    warped = along_y[0] + fz * slopes[0]
    resid = warped - current
    return warped, [resid * slope * (1.0 - t * t) for slope, t in zip(slopes, th)]


def main_kernel(
    slabs, cohort, own, peer, u0, offsets, template, wf, bxt, bx, wa, gather,
    total_out, delta_out,
    shifted, corners, grad, warped, current, moved, terms, grid, parts,
    small, piece, summed, pieces, means, wide, wide_means, peaks, mine,
    ex_send, ex_recv, pk_send, pk_recv, rs_send, rs_recv, tg_send, tg_recv,
    ag_send, ag_recv, fw_send, fw_recv, tl_send, tl_recv,
):
    me = lax.axis_index("slab")
    core = lax.axis_index("yslab")
    who = lax.axis_index("subj")
    other = 1 - core
    up = lax.rem(me + 1, slabs)
    down = lax.rem(me + slabs - 1, slabs)
    depth = offsets.shape[1]
    share = depth // cohort * 8
    barrier = pltpu.get_barrier_semaphore()
    each(1, slabs, lambda d: greet(barrier, slab=lax.rem(me + d, slabs)))
    each(1, cohort, lambda d: greet(barrier, subj=lax.rem(who + d, cohort)))
    greet(barrier, yslab=other)
    greet(barrier, slab=up, yslab=other)
    greet(barrier, slab=down, yslab=other)

    lane = lax.broadcasted_iota(jnp.int32, (8, 128), 1)
    below = core.astype(F32)
    above = 1.0 - below

    def build(z):
        out_low = jnp.logical_and(z < HALO, me == 0)
        out_high = jnp.logical_and(z >= depth + HALO, me == slabs - 1)
        keep = jnp.where(jnp.logical_or(out_low, out_high), 0.0, 1.0)
        for source, places in ((own, ((8, None),)), (peer, ((0, below), (16, above)))):
            plane = source[z].astype(F32) * keep
            a, b = plane[:, :128], plane[:, 128:]
            for move in range(-HALO, HALO + 1):
                if move == 0:
                    ra, rb = a, b
                else:
                    ra = pltpu.roll(a, (-move) % 128, 1)
                    rb = pltpu.roll(b, (-move) % 128, 1)
                    if move < 0:
                        ra, rb = (
                            jnp.where(lane < -move, 0.0, ra),
                            jnp.where(lane < -move, ra, rb),
                        )
                    else:
                        ra, rb = (
                            jnp.where(lane >= 128 - move, rb, ra),
                            jnp.where(lane >= 128 - move, 0.0, rb),
                        )
                for row, factor in places:
                    for half, value in enumerate((ra, rb)):
                        if factor is not None:
                            value = value * factor
                        shifted[move + HALO, z, half, row : row + 8, :] = value

    each(0, depth + 2 * HALO, build)

    def first_warp(z):
        rows = pl.ds(pl.multiple_of(z * 8, 8), 8)
        for half in range(2):
            cols = pl.ds(half * 128, 128)
            shift = []
            for c in range(3):
                value = offsets[c, z, :, cols]
                shift.append(((value & 1) == 1, value >= 0))
            planes = []
            for mz in range(5):
                lines = []
                for my in range(5):
                    values = [shifted[mx, z + mz, half, 6 + my : 14 + my, :] for mx in range(5)]
                    lines.append(list(pick(shift[2], values)))
                low, high = pick_many(shift[1], lines)
                planes.append(low + high)
            low, high = pick_many(shift[0], planes)
            found = low + high
            lows = found[0::2]
            steps = [found[2 * i + 1] - found[2 * i] for i in range(4)]
            for i in range(4):
                corners[i, rows, cols] = lows[i]
                corners[4 + i, rows, cols] = steps[i]
            u = [u0[c, rows, cols] for c in range(3)]
            value, slopes = warp(lows, steps, u, template[rows, cols])
            warped[rows, cols] = value
            for c in range(3):
                grad[c, rows, cols] = slopes[c]

    each(0, depth, first_warp)
    pl.semaphore_wait(barrier, slabs - 1 + cohort - 1 + 3)

    def part_of(ref, p):
        return ref.at[pl.ds(pl.multiple_of(p * share, share), share)]

    def scatter(it, source, slots):
        def copy(d):
            p = lax.rem(who + d, cohort)
            return send(
                part_of(source, p), slots.at[who], rs_send.at[it, d], rs_recv.at[it, who], subj=p
            )

        each(1, cohort, lambda d: copy(d).start())

        def recv():
            def one(d):
                p = lax.rem(who + d, cohort)
                send(
                    part_of(source, p), slots.at[p], rs_send.at[it, d], rs_recv.at[it, p], subj=p
                ).wait()

            each(1, cohort, one)

        return recv

    def spread(it, source, slots):
        each(
            1,
            cohort,
            lambda d: send(
                source, slots.at[who], tg_send.at[it, d], tg_recv.at[it, who],
                subj=lax.rem(who + d, cohort),
            ).start(),
        )

        def recv():
            def one(d):
                p = lax.rem(who + d, cohort)
                send(source, slots.at[p], tg_send.at[it, d], tg_recv.at[it, p], subj=p).wait()

            each(1, cohort, one)

        return recv

    def adjoint(it):
        for c in range(3):
            high, low = split(grad[c])
            first = dot(high, bx[...]) + dot(low, bx[...])
            high, low = split(first)
            part = dot(wa[...], jnp.concatenate([high, high, low], axis=0)) * SCALE
            cols = pl.ds(c * 128, 128)
            for g in range(3):
                terms[it, 3 * core + g, :, cols] = part[16 * g : 16 * g + 16].astype(BF16)

    def exchange(it):
        mine_rows = terms.at[it, pl.ds(3 * core, 3)]
        peer_rows = terms.at[it, pl.ds(3 * other, 3)]
        lower = terms.at[it, 3 * core]
        upper = terms.at[it, 3 * core + 1]
        plan = [
            (upper, 6, core, dict(slab=up)),
            (upper, 6, core, dict(slab=up, yslab=other)),
            (lower, 8, core, dict(slab=down)),
            (lower, 8, core, dict(slab=down, yslab=other)),
        ]
        outs = [
            send(src, terms.at[it, slot + k], ex_send.at[it, i], ex_recv.at[it, i], **where)
            for i, (src, slot, k, where) in enumerate(plan)
        ]
        ins = [
            send(src, terms.at[it, slot + k], ex_send.at[it, i], ex_recv.at[it, i], **where)
            for i, (src, slot, k, where) in enumerate(
                [
                    (upper, 6, core, dict(slab=up)),
                    (upper, 6, other, dict(slab=up, yslab=other)),
                    (lower, 8, core, dict(slab=down)),
                    (lower, 8, other, dict(slab=down, yslab=other)),
                ]
            )
        ]
        across = send(mine_rows, mine_rows, ex_send.at[it, 4], ex_recv.at[it, 4], yslab=other)
        back = send(mine_rows, peer_rows, ex_send.at[it, 4], ex_recv.at[it, 4], yslab=other)
        for copy in outs + [across]:
            copy.start()

        def recv():
            for copy in ins + [back]:
                copy.wait()

        return recv

    def reduce_terms(it):
        edge = jnp.where(me == 0, 1, jnp.where(me == slabs - 1, 2, 0))
        chosen = gather[edge]
        total = dot(chosen, terms[it].reshape(160, 384))
        grid[...] = total
        for q in range(4):
            parts[it, q] = total[16 * q : 16 * q + 16].astype(BF16)
        squares = total * total
        squares = squares[:, :128] + squares[:, 128:256] + squares[:, 256:]
        peak = jnp.sqrt(jnp.max(squares, axis=(0, 1), keepdims=True))
        mine[it] = jnp.broadcast_to(peak, (1, 128))

    def send_peaks(it):
        peaks[it, me] = mine[it]

        def start(d):
            slab = lax.rem(me + slabs - d, slabs)
            send(mine.at[it], peaks.at[it, me], pk_send.at[it, d], pk_recv.at[it, me], slab=slab).start()

        each(1, slabs, start)

        def recv():
            def one(d):
                slab = lax.rem(me + slabs - d, slabs)
                send(
                    mine.at[it], peaks.at[it, slab], pk_send.at[it, d], pk_recv.at[it, slab], slab=slab
                ).wait()

            each(1, slabs, one)
            peak = jnp.max(peaks[it], axis=0)
            return STEP / (peak + TINY)

        return recv

    def send_grid(it):
        block = parts.at[it, core]
        tail = parts.at[it, 2 + core]
        slot = 2 * me + core
        end = 2 * slabs + core
        last = me == slabs - 1

        def order(d):
            half = lax.div(d, 2)
            far = slabs // 2
            up_way = lax.rem(me + far - half, slabs)
            down_way = lax.rem(me + slabs - far + half, slabs)
            return jnp.where(lax.rem(d, 2) == 0, up_way, down_way)

        def start(d):
            slab = order(d)
            send(block, pieces.at[it, slot], ag_send.at[it, d], ag_recv.at[it, me], slab=slab).start()

        def start_tail(d):
            slab = order(d)
            send(tail, pieces.at[it, end], tl_send.at[it, d], tl_recv.at[it, 0], slab=slab).start()

        pieces[it, slot] = parts[it, core]

        @pl.when(last)
        def _():
            pieces[it, end] = parts[it, 2 + core]

        across = send(block, pieces.at[it, slot], fw_send.at[it, me], fw_recv.at[it, me], yslab=other)
        start(0)
        each(2, slabs, start)

        @pl.when(last)
        def _():
            start_tail(0)
            each(2, slabs, start_tail)

        across.start()

        def forward(d):
            slab = order(slabs + 1 - d)
            src = pieces.at[it, 2 * slab + core]
            send(block, src, ag_send.at[it, slabs + 1 - d], ag_recv.at[it, slab], slab=slab).wait()
            send(src, src, fw_send.at[it, slab], fw_recv.at[it, slab], yslab=other).start()

        def finish(d):
            slab = lax.rem(me + d, slabs)
            src = pieces.at[it, 2 * slab + core]
            dst = pieces.at[it, 2 * slab + other]
            send(src, dst, fw_send.at[it, slab], fw_recv.at[it, slab], yslab=other).wait()

        def recv():
            each(2, slabs, forward)
            far = order(0)
            src = pieces.at[it, 2 * far + core]
            send(block, src, ag_send.at[it, 0], ag_recv.at[it, far], slab=far).wait()
            send(src, src, fw_send.at[it, far], fw_recv.at[it, far], yslab=other).start()

            @pl.when(jnp.logical_not(last))
            def _():
                send(
                    tail, pieces.at[it, end], tl_send.at[it, 0], tl_recv.at[it, 0], slab=up
                ).wait_recv()

            src = pieces.at[it, end]
            send(src, src, fw_send.at[it, slabs], fw_recv.at[it, slabs], yslab=other).start()

            @pl.when(last)
            def _():
                send(tail, src, tl_send.at[it, 0], tl_recv.at[it, 0], slab=up).wait_send()
                each(
                    2,
                    slabs,
                    lambda d: send(
                        tail, src, tl_send.at[it, d], tl_recv.at[it, 0], slab=up
                    ).wait_send(),
                )

            each(0, slabs, finish)
            dst = pieces.at[it, 2 * slabs + other]
            send(src, dst, fw_send.at[it, slabs], fw_recv.at[it, slabs], yslab=other).wait()

        return recv

    def own_rows(ref):
        return ref[pl.ds(pl.multiple_of(who * share, share), share), :]

    small[...] = warped[...].astype(BF16)
    piece[who] = own_rows(small)
    got_parts = scatter(0, small, piece)
    adjoint(0)
    got_terms = exchange(0)
    got_terms()
    reduce_terms(0)
    got_peaks = send_peaks(0)
    got_grid_1 = send_grid(0)
    field([grid[:, c * 128 : c * 128 + 128] for c in range(3)], wf[core], bxt[...], moved)
    got_parts()
    total = piece[0].astype(F32)
    for p in range(1, cohort):
        total = total + piece[p].astype(F32)
    summed[...] = (total / cohort).astype(BF16)
    means[who] = summed[...]
    got_means = spread(0, summed, means)
    factor_1 = got_peaks()
    got_means()
    for p in range(cohort):
        current[p * share : p * share + share] = means[p].astype(F32)

    def second_warp(z):
        rows = pl.ds(pl.multiple_of(z * 8, 8), 8)
        for half in range(2):
            cols = pl.ds(half * 128, 128)
            lows = [corners[i, rows, cols] for i in range(4)]
            steps = [corners[4 + i, rows, cols] for i in range(4)]
            u = [u0[c, rows, cols] - factor_1 * moved[c, rows, cols] for c in range(3)]
            value, slopes = warp(lows, steps, u, current[rows, cols])
            warped[rows, cols] = value
            for c in range(3):
                grad[c, rows, cols] = slopes[c]

    each(0, depth, second_warp)
    wide[who] = own_rows(warped)
    got_parts = scatter(1, warped, wide)
    adjoint(1)
    got_terms = exchange(1)
    got_terms()
    reduce_terms(1)
    got_peaks = send_peaks(1)
    got_grid_2 = send_grid(1)
    got_parts()
    total = wide[0]
    for p in range(1, cohort):
        total = total + wide[p]
    current[0:share] = total
    wide_means[who] = total
    got_means = spread(1, current.at[pl.ds(0, share)], wide_means)
    got_grid_1()
    factor_2 = got_peaks()
    got_grid_2()

    def combine(t):
        change = factor_1[:, 0:1] * pieces[0, t].astype(F32) + factor_2[:, 0:1] * pieces[1, t].astype(F32)
        for c in range(3):
            for i in range(2):
                delta_out[c, 2 * t + i] = change[8 * i : 8 * i + 8, c * 128 : c * 128 + 128]

    each(0, 2 * slabs + 2, combine)
    got_means()
    for p in range(cohort):
        total_out[p * share : p * share + share] = wide_means[p]


def call(kernel, name, outs, scratch, ident, args, spaces):
    return pl.pallas_call(
        kernel,
        out_shape=outs,
        in_specs=[pl.BlockSpec(memory_space=s) for s in spaces],
        out_specs=[pl.BlockSpec(memory_space=pltpu.VMEM)] * len(outs),
        scratch_shapes=scratch,
        compiler_params=pltpu.CompilerParams(
            collective_id=ident, has_side_effects=True, vmem_limit_bytes=24 * 1024 * 1024
        ),
        name=name,
    )(*args)


def solution(mesh):
    slabs = mesh.shape["slab"]
    cohort = mesh.shape["subj"]
    assert mesh.shape["yslab"] == 2 and slabs >= 4 and slabs % 2 == 0

    def shards(subjects, offsets, template, control):
        depth, height, width = subjects.shape[1:]
        rows = depth * height
        share = rows // cohort
        wf, bxt, bx, wa, gather = constants(depth, height, width, control.shape[4])
        vmem = pltpu.VMEM
        dma = pltpu.SemaphoreType.DMA
        deep = depth + 2 * HALO
        own, peer, u0 = call(
            lambda *refs: halo_kernel(slabs, *refs),
            "halo",
            [
                jax.ShapeDtypeStruct((deep, height, width), BF16),
                jax.ShapeDtypeStruct((deep, height, width), BF16),
                jax.ShapeDtypeStruct((3, rows, width), F32),
            ],
            [
                vmem((deep, height, width), BF16),
                vmem((deep, height, width), BF16),
                vmem((3, 7, 7, 128), F32),
                vmem((3, 8, 8, 128), F32),
                dma,
                dma((5,)),
                dma((5,)),
            ],
            0,
            (subjects[0], control[0], wf, bxt),
            (vmem, pl.ANY, vmem, vmem),
        )
        total, delta = call(
            lambda *refs: main_kernel(slabs, cohort, *refs),
            "main",
            [
                jax.ShapeDtypeStruct((rows, width), F32),
                jax.ShapeDtypeStruct((3, 4 * slabs + 4, 8, 128), F32),
            ],
            [
                vmem((5, deep, 2, 24, 128), F32),
                vmem((8, rows, width), F32),
                vmem((3, rows, width), F32),
                vmem((rows, width), F32),
                vmem((rows, width), F32),
                vmem((3, rows, width), F32),
                vmem((2, 10, 16, 384), BF16),
                vmem((64, 384), F32),
                vmem((2, 4, 16, 384), BF16),
                vmem((rows, width), BF16),
                vmem((cohort, share, width), BF16),
                vmem((share, width), BF16),
                vmem((2, 2 * slabs + 2, 16, 384), BF16),
                vmem((cohort, share, width), BF16),
                vmem((cohort, share, width), F32),
                vmem((cohort, share, width), F32),
                vmem((2, slabs, 1, 128), F32),
                vmem((2, 1, 128), F32),
                dma((2, 5)), dma((2, 5)),
                dma((2, slabs)), dma((2, slabs)),
                dma((2, cohort)), dma((2, cohort)),
                dma((2, cohort)), dma((2, cohort)),
                dma((2, slabs)), dma((2, slabs)),
                dma((2, slabs + 1)), dma((2, slabs + 1)),
                dma((2, slabs)), dma((2, 1)),
            ],
            1,
            (own, peer, u0, offsets[0], template.reshape(rows, width), wf, bxt, bx, wa, gather),
            (vmem,) * 10,
        )
        template_out = (total / cohort).reshape(depth, height, width)
        control_out = control - delta[None, :, : control.shape[2], : control.shape[3], :]
        return template_out, control_out

    in_specs = (
        P(("group", "subj"), "slab", "yslab", None),
        P(("group", "subj"), None, "slab", "yslab", None),
        P(("group", "slab"), "yslab", None),
        P(("group", "subj"), None, None, None, None),
    )
    out_specs = (P(("group", "slab"), "yslab", None), P(("group", "subj"), None, None, None, None))
    return jax.shard_map(shards, mesh=mesh, in_specs=in_specs, out_specs=out_specs, check_vma=False)
```

```python
import jax
import jax.numpy as jnp
import numpy as np
from jax import lax
from jax.experimental import pallas as pl
from jax.experimental.pallas import tpu as pltpu
from jax.sharding import PartitionSpec as P

KNOT = 4
HALO = 2
STEP = 0.5
TINY = 1e-06
CUBE = 384.0
CUBE_X = 48.0
SCALE = 1.0 / (CUBE * CUBE * CUBE_X)
F32 = jnp.float32
BF16 = jnp.bfloat16
MESH = pl.DeviceIdType.MESH


def spline(count, columns, spacing, wrap):
    whole = 6 * spacing**3
    matrix = np.zeros((count, columns))
    for t in range(count):
        j = t // spacing
        s = (t - j * spacing) / spacing
        weights = [
            (1 - s) ** 3 / 6,
            (3 * s**3 - 6 * s**2 + 4) / 6,
            (-3 * s**3 + 3 * s**2 + 3 * s + 1) / 6,
            s**3 / 6,
        ]
        for o in range(4):
            column = (j + o) % columns if wrap else j + o
            matrix[t, column] += weights[o] * whole
    return np.rint(matrix)


def halves(whole):
    high = np.asarray(whole, np.float32).astype(BF16).astype(np.float32)
    low = (whole - high).astype(np.float32)
    assert (low.astype(BF16).astype(np.float32) == low).all()
    return high, low


def constants(depth, height, width, columns_x):
    assert (depth, height) == (16, 8)
    bz = spline(depth, 7, KNOT, False)
    by = spline(height, 5, KNOT, False)
    forward = np.zeros((2, depth, height, 8, 8))
    for k in range(2):
        forward[k, :, :, :7, 2 * k : 2 * k + 5] = np.einsum("za,yb->zyab", bz, by)
    dense = np.zeros((2, 2, depth * height, 64))
    rows = forward[:, :, :, :7, :7].reshape(2, depth * height, 49)
    dense[:, 0, :, :49] = rows
    dense[:, 1, :, 7:56] = rows
    forward = forward.reshape(2, depth * height, 64)
    forward = np.concatenate([dense, forward[:, None]], axis=1)
    high, low = halves(forward)
    forward = np.concatenate([high, low, high], axis=3)
    adjoint = np.zeros((3, 16, depth, height))
    for group, rows in enumerate(([0, 1, 2], [4, 5, 6], [3])):
        for place, a in enumerate(rows):
            for b in range(5):
                adjoint[group, place * 5 + b] = np.outer(bz[:, a], by[:, b])
    adjoint = adjoint.reshape(48, depth * height)
    high, low = halves(adjoint)
    adjoint = np.concatenate([high, low, high], axis=1)
    gather = np.zeros((3, 64, 10, 16))
    for edge in range(3):
        for a in range(7):
            for b in range(7):
                for k in range(2):
                    c = b - 2 * k
                    if not 0 <= c < 5:
                        continue
                    row = a * 8 + b
                    if a < 3:
                        gather[edge, row, 3 * k, a * 5 + c] = 1
                        if edge != 1:
                            gather[edge, row, 6 + k, a * 5 + c] = 1
                    elif a == 3:
                        gather[edge, row, 3 * k + 2, c] = 1
                    else:
                        gather[edge, row, 3 * k + 1, (a - 4) * 5 + c] = 1
                        if edge != 2:
                            gather[edge, row, 8 + k, (a - 4) * 5 + c] = 1
    gather = gather.reshape(3, 64, 160)
    bx = spline(width, columns_x, 2, True)
    across = np.concatenate([bx.T, bx.T], axis=0)
    bx = np.concatenate([bx, bx], axis=0)
    return [jnp.asarray(m, BF16) for m in (forward, across, bx, adjoint, gather)]


def split(x):
    high = x.astype(BF16)
    return high, (x - high.astype(F32)).astype(BF16)


def dot(a, b):
    return jnp.dot(a, b, preferred_element_type=F32)


def field(coeffs, wf, bxt, out):
    high, low = split(coeffs)
    first = dot(wf, jnp.concatenate([high, high, low], axis=0))
    high, low = split(first)
    for c in range(3):
        cols = slice(c * 128, c * 128 + 128)
        out[c] = dot(jnp.concatenate([high[:, cols], low[:, cols]], axis=1), bxt) * SCALE


def send(src, dst, send_sem, recv_sem, **where):
    return pltpu.make_async_remote_copy(
        src_ref=src,
        dst_ref=dst,
        send_sem=send_sem,
        recv_sem=recv_sem,
        device_id=where,
        device_id_type=MESH,
    )


def greet(barrier, **where):
    pl.semaphore_signal(barrier, inc=1, device_id=where, device_id_type=MESH)


def wait_in(ref, sem, **where):
    send(ref, ref, sem, sem, **where).wait_recv()


def wait_out(ref, sem, **where):
    send(ref, ref, sem, sem, **where).wait_send()


def each(first, last, body):
    def step(i, carry):
        body(i)
        return carry

    lax.fori_loop(first, last, step, 0)


def pick(shift, values):
    odd, top = shift
    steps = [jnp.where(odd, values[i + 1], values[i]) for i in range(4)]
    return jnp.where(top, steps[2], steps[0]), jnp.where(top, steps[3], steps[1])


def pick_many(shift, groups):
    pairs = [pick(shift, values) for values in zip(*groups)]
    return [p[0] for p in pairs], [p[1] for p in pairs]


def warp(lows, steps, u, current):
    th = [jnp.tanh(x) for x in u]
    fz, fy, fx = [0.5 + 0.5 * t for t in th]
    along = [low + fx * step for low, step in zip(lows, steps)]
    slope_y = [along[1] - along[0], along[3] - along[2]]
    along_y = [along[0] + fy * slope_y[0], along[2] + fy * slope_y[1]]
    slope_x = [steps[0] + fy * (steps[1] - steps[0]), steps[2] + fy * (steps[3] - steps[2])]
    slopes = [
        along_y[1] - along_y[0],
        slope_y[0] + fz * (slope_y[1] - slope_y[0]),
        slope_x[0] + fz * (slope_x[1] - slope_x[0]),
    ]
    warped = along_y[0] + fz * slopes[0]
    resid = warped - current
    return warped, [resid * slope * (1.0 - t * t) for slope, t in zip(slopes, th)]


def main_kernel(
    slabs, cohort, subject, offsets_in, template_in, control, wf_in, bxt_in, bx_in, wa_in, gather_in,
    mean_out, delta_out,
    own, peer, band, u0, offsets, template, wf, bxt, bx, wa, gather,
    shifted, corners, grad, warped, current, moved, terms, grid,
    small, piece, summed, pieces, means, wide, wide_means, peaks, mine,
    in_sem, halo_sem, know_sem, know_subj_sem, ex_sem, pk_sem, rs_sem, tg_sem, ag_sem, fw_sem,
):
    me = lax.axis_index("slab")
    core = lax.axis_index("yslab")
    who = lax.axis_index("subj")
    other = 1 - core
    depth = offsets.shape[1]
    share = depth // cohort * 8
    far = slabs // 2
    hop = slabs // 4

    def slab_at(d):
        return lax.rem(me + (d + slabs), slabs)

    def subj_at(d):
        return lax.rem(who + (d + cohort), cohort)

    up, down = slab_at(1), slab_at(-1)
    barrier = pltpu.get_barrier_semaphore()
    greet(barrier, yslab=other)
    for slab in (up, down):
        greet(barrier, slab=slab)
        greet(barrier, slab=slab, yslab=other)
    for d in (1, -1):
        greet(barrier, subj=subj_at(d))

    rows_in = control.shape[0] // 3
    begin = jnp.minimum(me * (depth // KNOT * 7), rows_in - 56)
    late = jnp.where(me == slabs - 1, 1, 0)
    inner = pl.ds(HALO, depth)
    fetch_subject = pltpu.make_async_copy(subject, own.at[inner], in_sem.at[0])
    fetch_control = [
        pltpu.make_async_copy(
            control.at[pl.ds(c * rows_in + begin, 56), 0],
            band.at[pl.ds(0, 56), pl.ds(c * 128, 128)],
            in_sem.at[1 + c],
        )
        for c in range(3)
    ]
    fetch_rest = [
        pltpu.make_async_copy(src, dst, in_sem.at[4 + i])
        for i, (src, dst) in enumerate(
            [
                (wf_in.at[core, late], wf.at[0]),
                (bxt_in, bxt),
                (wf_in.at[core, 2], wf.at[1]),
                (offsets_in, offsets),
                (template_in, template),
                (bx_in, bx),
                (wa_in, wa),
                (gather_in, gather),
            ]
        )
    ]
    for copy in [fetch_subject] + fetch_control + fetch_rest:
        copy.start()
    band[56:64, :] = jnp.zeros((8, 384), F32)

    pl.semaphore_wait(barrier, 7)
    fetch_subject.wait()
    low = pl.ds(0, HALO)
    high = pl.ds(depth + HALO, HALO)
    first = pl.ds(HALO, HALO)
    last = pl.ds(depth, HALO)
    across = send(own.at[inner], peer.at[inner], halo_sem.at[0], halo_sem.at[1], yslab=other)
    along = [
        send(own.at[last], own.at[low], halo_sem.at[2], halo_sem.at[3], slab=up),
        send(own.at[first], own.at[high], halo_sem.at[2], halo_sem.at[3], slab=down),
        send(own.at[last], peer.at[low], halo_sem.at[2], halo_sem.at[3], slab=up, yslab=other),
        send(own.at[first], peer.at[high], halo_sem.at[2], halo_sem.at[3], slab=down, yslab=other),
    ]
    for copy in along + [across]:
        copy.start()

    know_slab = [1]
    know_subj = [1]

    def tell():
        if know_slab[0] < far:
            r = know_slab[0].bit_length() - 1
            for d in (know_slab[0], -know_slab[0]):
                greet(know_sem.at[r], slab=slab_at(d))
        if know_subj[0] < cohort // 2:
            r = know_subj[0].bit_length() - 1
            for d in (know_subj[0], -know_subj[0]):
                greet(know_subj_sem.at[r], subj=subj_at(d))

    def learn():
        if know_slab[0] < far:
            pl.semaphore_wait(know_sem.at[know_slab[0].bit_length() - 1], 2)
            know_slab[0] *= 2
        if know_subj[0] < cohort // 2:
            pl.semaphore_wait(know_subj_sem.at[know_subj[0].bit_length() - 1], 2)
            know_subj[0] *= 2

    tell()

    for copy in fetch_control + fetch_rest[:2]:
        copy.wait()
    field(band[...], wf[0], bxt[...], u0)

    lane = lax.broadcasted_iota(jnp.int32, (8, 128), 1)
    below = core.astype(F32)
    above = 1.0 - below

    def build(source, places, z):
        out_low = jnp.logical_and(z < HALO, me == 0)
        out_high = jnp.logical_and(z >= depth + HALO, me == slabs - 1)
        keep = jnp.where(jnp.logical_or(out_low, out_high), 0.0, 1.0)
        plane = source[z].astype(F32) * keep
        a, b = plane[:, :128], plane[:, 128:]
        for move in range(-HALO, HALO + 1):
            if move == 0:
                ra, rb = a, b
            else:
                ra = pltpu.roll(a, (-move) % 128, 1)
                rb = pltpu.roll(b, (-move) % 128, 1)
                if move < 0:
                    ra, rb = (
                        jnp.where(lane < -move, 0.0, ra),
                        jnp.where(lane < -move, ra, rb),
                    )
                else:
                    ra, rb = (
                        jnp.where(lane >= 128 - move, rb, ra),
                        jnp.where(lane >= 128 - move, 0.0, rb),
                    )
            for row, factor in places:
                for half, value in enumerate((ra, rb)):
                    if factor is not None:
                        value = value * factor
                    shifted[move + HALO, z, half, row : row + 8, :] = value

    at_own = ((8, None),)
    at_peer = ((0, below), (16, above))

    def edge_of(i, top):
        return jnp.where(i < HALO, i, i + (top - HALO))

    each(HALO, depth + HALO, lambda z: build(own, at_own, z))
    learn()
    tell()
    across.wait()
    each(HALO, depth + HALO, lambda z: build(peer, at_peer, z))
    for copy in fetch_rest[2:]:
        copy.wait()

    def first_warp(z):
        rows = pl.ds(pl.multiple_of(z * 8, 8), 8)
        for half in range(2):
            cols = pl.ds(half * 128, 128)
            shift = []
            for c in range(3):
                value = offsets[c, z, :, cols]
                shift.append(((value & 1) == 1, value >= 0))
            planes = []
            for mz in range(5):
                lines = []
                for my in range(5):
                    values = [shifted[mx, z + mz, half, 6 + my : 14 + my, :] for mx in range(5)]
                    lines.append(list(pick(shift[2], values)))
                low, high = pick_many(shift[1], lines)
                planes.append(low + high)
            low, high = pick_many(shift[0], planes)
            found = low + high
            lows = found[0::2]
            steps = [found[2 * i + 1] - found[2 * i] for i in range(4)]
            for i in range(4):
                corners[i, rows, cols] = lows[i]
                corners[4 + i, rows, cols] = steps[i]
            u = [u0[c, rows, cols] for c in range(3)]
            value, slopes = warp(lows, steps, u, template[rows, cols])
            warped[rows, cols] = value
            for c in range(3):
                grad[c, rows, cols] = slopes[c]

    each(HALO, depth - HALO, first_warp)
    learn()
    tell()
    planes = own.at[pl.ds(0, 4 * HALO)]
    wait_in(planes, halo_sem.at[3], slab=up)
    wait_out(planes, halo_sem.at[2], slab=up)

    def build_edge(i):
        z = edge_of(i, depth + HALO)
        build(own, at_own, z)
        build(peer, at_peer, z)

    each(0, 2 * HALO, build_edge)
    each(0, 2 * HALO, lambda i: first_warp(edge_of(i, depth - HALO)))
    while know_subj[0] < cohort // 2:
        learn()
        tell()

    def part_of(ref, p):
        return ref.at[pl.ds(pl.multiple_of(p * share, share), share)]

    def own_rows(ref):
        return ref[pl.ds(pl.multiple_of(who * share, share), share), :]

    others = [d for d in range(1, cohort)]

    def scatter(it, source, slots):
        for d in others:
            p = subj_at(d)
            send(part_of(source, p), slots.at[who], rs_sem.at[it, 0], rs_sem.at[it, 1], subj=p).start()

    def spread(it, source, slots):
        for d in others:
            send(source, slots.at[who], tg_sem.at[it, 0], tg_sem.at[it, 1], subj=subj_at(d)).start()

    def got(it, slots, sem):
        several = slots.at[pl.ds(0, cohort - 1)]
        wait_in(several, sem.at[it, 1], subj=subj_at(1))
        wait_out(several, sem.at[it, 0], subj=subj_at(1))

    def adjoint(it):
        firsts = []
        for c in range(3):
            high, low = split(grad[c])
            firsts.append(dot(jnp.concatenate([high, low], axis=1), bx[...]))
        high, low = split(jnp.concatenate(firsts, axis=1))
        part = dot(wa[...], jnp.concatenate([high, high, low], axis=0)) * SCALE
        for g in range(3):
            terms[it, 3 * core + g] = part[16 * g : 16 * g + 16].astype(BF16)

    def exchange(it):
        mine_rows = terms.at[it, pl.ds(3 * core, 3)]
        lower = terms.at[it, 3 * core]
        upper = terms.at[it, 3 * core + 1]
        sems = (ex_sem.at[it, 0], ex_sem.at[it, 1])
        send(upper, terms.at[it, 6 + core], *sems, slab=up, yslab=other).start()
        send(lower, terms.at[it, 8 + core], *sems, slab=down, yslab=other).start()
        send(upper, terms.at[it, 6 + core], *sems, slab=up).start()
        send(lower, terms.at[it, 8 + core], *sems, slab=down).start()
        send(mine_rows, mine_rows, *sems, yslab=other).start()

    def got_exchange(it):
        several = terms.at[it, pl.ds(0, 7)]
        wait_in(several, ex_sem.at[it, 1], yslab=other)
        wait_out(several, ex_sem.at[it, 0], yslab=other)

    def reduce_terms(it):
        edge = jnp.where(me == 0, 1, jnp.where(me == slabs - 1, 2, 0))
        total = dot(gather[edge], terms[it].reshape(160, 384))
        squares = total * total
        squares = squares[:, :128] + squares[:, 128:256] + squares[:, 256:]
        peak = jnp.sqrt(jnp.max(squares, axis=(0, 1), keepdims=True))
        mine[...] = jnp.broadcast_to(peak, (1, 128))
        p0 = peak.astype(BF16).astype(F32)
        p1 = (peak - p0).astype(BF16).astype(F32)
        p2 = peak - p0 - p1
        wide_peak = jnp.concatenate([jnp.broadcast_to(p, (64, 128)) for p in (p0, p1, p2)], axis=1)
        row = lax.broadcasted_iota(jnp.int32, (64, 384), 0)
        packed = jnp.where((row & 7) == 7, wide_peak, total).astype(BF16)
        grid[...] = total
        lowest = packed[0:16], packed[32:48]
        highest = packed[16:32], packed[48:64]
        pieces[it, core, me] = jnp.where(core == 0, lowest[0], highest[0])

        @pl.when(me == slabs - 1)
        def _():
            pieces[it, core, slabs] = jnp.where(core == 0, lowest[1], highest[1])

    def send_peaks():
        peaks[me] = mine[...]
        for i in range(slabs - 1):
            d = far if i == 0 else (far - (i + 1) // 2) * (1 if i % 2 else -1)
            send(mine, peaks.at[me], pk_sem.at[0], pk_sem.at[1], slab=slab_at(d)).start()

    def got_peaks():
        several = peaks.at[pl.ds(0, slabs - 1)]
        wait_in(several, pk_sem.at[1], slab=up)
        wait_out(several, pk_sem.at[0], slab=up)
        return STEP / (jnp.max(peaks[...], axis=0) + TINY)

    end = slabs - 1

    def blocks(it, origin, count):
        return pieces.at[it, core, pl.ds(origin, count)]

    def ship(it, origin, sent, targets):
        for ends, count in ((origin == end, 2), (origin != end, 1)):

            @pl.when(ends)
            def _():
                ref = blocks(it, origin, count)
                for d, place in targets:
                    send(ref, ref, ag_sem.at[it, sent], ag_sem.at[it, place], slab=slab_at(d)).start()

    def settle(it, count, extra, origins, wait, place):
        found = origins[0] == end
        for origin in origins[1:]:
            found = jnp.logical_or(found, origin == end)
        for case, number in ((found, count + extra), (jnp.logical_not(found), count)):

            @pl.when(case)
            def _():
                wait(blocks(it, 0, number), ag_sem.at[it, place], slab=up)

    OWN, EDGE_UP, EDGE_DOWN, NEAR, FAR, GO_UP, GO_DOWN = range(7)

    def send_grid(it):
        targets = [(hop, EDGE_UP), (-hop, EDGE_DOWN)]
        for d in range(hop - 1, 0, -1):
            targets += [(d, NEAR), (-d, NEAR)]
        ship(it, me, OWN, targets)

    def hand_on(it):
        origin = slab_at(-hop)
        settle(it, 1, 1, [origin], wait_in, EDGE_UP)
        ship(it, origin, GO_UP, [(d, FAR) for d in range(hop, 0, -1)])
        origin = slab_at(hop)
        settle(it, 1, 1, [origin], wait_in, EDGE_DOWN)
        ship(it, origin, GO_DOWN, [(-d, FAR) for d in range(hop - 1, 0, -1)])

    def got_grid(it):
        near = [slab_at(d) for d in range(1 - hop, hop) if d != 0]
        if near:
            settle(it, len(near), 1, near, wait_in, NEAR)
        distant = [slab_at(d) for d in range(hop + 1, slabs - hop)]
        settle(it, len(distant), 1, distant, wait_in, FAR)
        both = pieces.at[it, core]
        send(both, both, fw_sem.at[it, 0], fw_sem.at[it, 1], yslab=other).start()

    def sent_grid(it):
        both = pieces.at[it, core]
        send(both, both, fw_sem.at[it, 0], fw_sem.at[it, 1], yslab=other).wait()
        for origin, count, sent in (
            (me, 2 * hop, OWN),
            (slab_at(-hop), hop, GO_UP),
            (slab_at(hop), hop - 1, GO_DOWN),
        ):
            if count:
                settle(it, count, count, [origin], wait_out, sent)

    small[...] = warped[...].astype(BF16)
    piece[who] = own_rows(small)
    scatter(0, small, piece)
    adjoint(0)
    exchange(0)
    while know_slab[0] < far:
        learn()
        tell()
    got_exchange(0)
    reduce_terms(0)
    send_peaks()
    send_grid(0)
    field(grid[...], wf[1], bxt[...], moved)
    got(0, piece, rs_sem)
    total = piece[0].astype(F32)
    for p in range(1, cohort):
        total = total + piece[p].astype(F32)
    summed[...] = (total / cohort).astype(BF16)
    means[who] = summed[...]
    spread(0, summed, means)
    hand_on(0)
    factor_1 = got_peaks()
    got(0, means, tg_sem)
    for p in range(cohort):
        current[p * share : p * share + share] = means[p].astype(F32)

    def second_warp(z):
        rows = pl.ds(pl.multiple_of(z * 8, 8), 8)
        for half in range(2):
            cols = pl.ds(half * 128, 128)
            lows = [corners[i, rows, cols] for i in range(4)]
            steps = [corners[4 + i, rows, cols] for i in range(4)]
            u = [u0[c, rows, cols] - factor_1 * moved[c, rows, cols] for c in range(3)]
            value, slopes = warp(lows, steps, u, current[rows, cols])
            warped[rows, cols] = value
            for c in range(3):
                grad[c, rows, cols] = slopes[c]

    each(0, depth, second_warp)
    wide[who] = own_rows(warped)
    adjoint(1)
    exchange(1)
    scatter(1, warped, wide)
    got_exchange(1)
    reduce_terms(1)
    send_grid(1)
    got_grid(0)
    got(1, wide, rs_sem)
    total = wide[0]
    for p in range(1, cohort):
        total = total + wide[p]
    total = total / cohort
    current[0:share] = total
    wide_means[who] = total
    spread(1, current.at[pl.ds(0, share)], wide_means)
    hand_on(1)
    sent_grid(0)
    got_grid(1)
    got(1, wide_means, tg_sem)
    for p in range(cohort):
        mean_out[p * share : p * share + share] = wide_means[p]
    sent_grid(1)

    peak = None
    for k in range(2):
        for slab in range(slabs):
            row = pieces[1, k, slab, 7:8, :].astype(F32)
            row = (row[:, :128] + row[:, 128:256]) + row[:, 256:]
            peak = row if peak is None else jnp.maximum(peak, row)
    factor_2 = STEP / (peak + TINY)
    grid_rows = delta_out.shape[0] // 21
    sub = lax.broadcasted_iota(jnp.int32, (8, 128), 0)
    made = {}

    def change(s):
        if s not in made:
            c, a = divmod(s, grid_rows)
            cols = slice(c * 128, c * 128 + 128)
            k, slab, i = (a // 2) % 2, a // 4, a % 2
            one, two = (
                pieces[it, k, slab, :, cols].astype(F32)[8 * i : 8 * i + 8] for it in range(2)
            )
            made[s] = factor_1 * one + factor_2 * two
        return made[s]

    for t in range((3 * grid_rows * 7 + 7) // 8):
        s, skip = divmod(8 * t, 7)
        value = change(s)
        if skip:
            value = pltpu.roll(value, 8 - skip, 0)
        if s + 1 < 3 * grid_rows:
            after = change(s + 1)
            if skip < 6:
                pass
            after = pltpu.roll(after, 7 - skip, 0)
            value = jnp.where(sub < 7 - skip, value, after)
            delta_out[8 * t : 8 * t + 8, :] = value
        else:
            delta_out[8 * t : 8 * t + 7 - skip, :] = value[0 : 7 - skip]
        made.pop(s - 1, None)


def solution(mesh):
    slabs = mesh.shape["slab"]
    cohort = mesh.shape["subj"]
    assert mesh.shape["yslab"] == 2 and slabs >= 4 and slabs % 4 == 0

    def shards(subjects, offsets, template, control):
        depth, height, width = subjects.shape[1:]
        rows = depth * height
        share = rows // cohort
        wf, bxt, bx, wa, gather = constants(depth, height, width, control.shape[4])
        vmem = pltpu.VMEM
        dma = pltpu.SemaphoreType.DMA
        plain = pltpu.SemaphoreType.REGULAR
        deep = depth + 2 * HALO
        grid_rows = control.shape[2]
        rounds = (slabs // 2).bit_length() - 1
        args = (
            subjects[0],
            offsets[0],
            template.reshape(rows, width),
            control.reshape(3 * grid_rows * 7, 1, 128),
            wf, bxt, bx, wa, gather,
        )
        mean, delta = pl.pallas_call(
            lambda *refs: main_kernel(slabs, cohort, *refs),
            out_shape=[
                jax.ShapeDtypeStruct((rows, width), F32),
                jax.ShapeDtypeStruct((3 * grid_rows * 7, 128), F32),
            ],
            in_specs=[pl.BlockSpec(memory_space=pl.ANY)] * len(args),
            out_specs=[pl.BlockSpec(memory_space=vmem)] * 2,
            scratch_shapes=[
                vmem((deep, height, width), BF16),
                vmem((deep, height, width), BF16),
                vmem((64, 384), F32),
                vmem((3, rows, width), F32),
                vmem((3, depth, height, width), jnp.int32),
                vmem((rows, width), F32),
                vmem((2, *wf.shape[2:]), BF16),
                vmem(bxt.shape, BF16),
                vmem(bx.shape, BF16),
                vmem(wa.shape, BF16),
                vmem(gather.shape, BF16),
                vmem((5, deep, 2, 24, 128), F32),
                vmem((8, rows, width), F32),
                vmem((3, rows, width), F32),
                vmem((rows, width), F32),
                vmem((rows, width), F32),
                vmem((3, rows, width), F32),
                vmem((2, 10, 16, 384), BF16),
                vmem((64, 384), F32),
                vmem((rows, width), BF16),
                vmem((cohort, share, width), BF16),
                vmem((share, width), BF16),
                vmem((2, 2, slabs + 1, 16, 384), BF16),
                vmem((cohort, share, width), BF16),
                vmem((cohort, share, width), F32),
                vmem((cohort, share, width), F32),
                vmem((slabs, 1, 128), F32),
                vmem((1, 128), F32),
                dma((12,)),
                dma((4,)),
                plain((rounds,)),
                plain((max((cohort // 2).bit_length() - 1, 1),)),
                dma((2, 2)),
                dma((2,)),
                dma((2, 2)),
                dma((2, 2)),
                dma((2, 7)),
                dma((2, 2)),
            ],
            compiler_params=pltpu.CompilerParams(
                collective_id=0, has_side_effects=True, vmem_limit_bytes=48 * 1024 * 1024
            ),
            name="register",
        )(*args)
        return mean.reshape(depth, height, width), control - delta.reshape(control.shape)

    in_specs = (
        P(("group", "subj"), "slab", "yslab", None),
        P(("group", "subj"), None, "slab", "yslab", None),
        P(("group", "slab"), "yslab", None),
        P(("group", "subj"), None, None, None, None),
    )
    out_specs = (P(("group", "slab"), "yslab", None), P(("group", "subj"), None, None, None, None))
    return jax.shard_map(shards, mesh=mesh, in_specs=in_specs, out_specs=out_specs, check_vma=False)
```

```python
import jax
import jax.numpy as jnp
import numpy as np
from jax import lax
from jax.experimental import pallas as pl
from jax.experimental.pallas import tpu as pltpu
from jax.sharding import PartitionSpec as P

KNOT = 4
HALO = 2
STEP = 0.5
TINY = 1e-06
CUBE = 384.0
CUBE_X = 48.0
SCALE = 1.0 / (CUBE * CUBE * CUBE_X)
F32 = jnp.float32
BF16 = jnp.bfloat16
MESH = pl.DeviceIdType.MESH


def spline(count, columns, spacing, wrap):
    whole = 6 * spacing**3
    matrix = np.zeros((count, columns))
    for t in range(count):
        j = t // spacing
        s = (t - j * spacing) / spacing
        weights = [
            (1 - s) ** 3 / 6,
            (3 * s**3 - 6 * s**2 + 4) / 6,
            (-3 * s**3 + 3 * s**2 + 3 * s + 1) / 6,
            s**3 / 6,
        ]
        for o in range(4):
            column = (j + o) % columns if wrap else j + o
            matrix[t, column] += weights[o] * whole
    return np.rint(matrix)


def halves(whole):
    high = np.asarray(whole, np.float32).astype(BF16).astype(np.float32)
    low = (whole - high).astype(np.float32)
    assert (low.astype(BF16).astype(np.float32) == low).all()
    return high, low


def constants(depth, height, width, columns_x):
    assert (depth, height) == (16, 8)
    bz = spline(depth, 7, KNOT, False)
    by = spline(height, 5, KNOT, False)
    forward = np.zeros((2, depth, height, 8, 8))
    for k in range(2):
        forward[k, :, :, :7, 2 * k : 2 * k + 5] = np.einsum("za,yb->zyab", bz, by)
    dense = np.zeros((2, 2, depth * height, 64))
    rows = forward[:, :, :, :7, :7].reshape(2, depth * height, 49)
    dense[:, 0, :, :49] = rows
    dense[:, 1, :, 7:56] = rows
    forward = forward.reshape(2, depth * height, 64)
    forward = np.concatenate([dense, forward[:, None]], axis=1)
    high, low = halves(forward)
    forward = np.concatenate([high, low, high], axis=3)
    adjoint = np.zeros((3, 16, depth, height))
    for group, rows in enumerate(([0, 1, 2], [4, 5, 6], [3])):
        for place, a in enumerate(rows):
            for b in range(5):
                adjoint[group, place * 5 + b] = np.outer(bz[:, a], by[:, b])
    adjoint = adjoint.reshape(48, depth * height)
    high, low = halves(adjoint)
    adjoint = np.concatenate([high, low, high], axis=1)
    gather = np.zeros((3, 64, 10, 16))
    for edge in range(3):
        for a in range(7):
            for b in range(7):
                for k in range(2):
                    c = b - 2 * k
                    if not 0 <= c < 5:
                        continue
                    row = a * 8 + b
                    if a < 3:
                        gather[edge, row, 3 * k, a * 5 + c] = 1
                        if edge != 1:
                            gather[edge, row, 6 + k, a * 5 + c] = 1
                    elif a == 3:
                        gather[edge, row, 3 * k + 2, c] = 1
                    else:
                        gather[edge, row, 3 * k + 1, (a - 4) * 5 + c] = 1
                        if edge != 2:
                            gather[edge, row, 8 + k, (a - 4) * 5 + c] = 1
    gather = gather.reshape(3, 64, 160)
    bx = spline(width, columns_x, 2, True)
    across = np.concatenate([bx.T, bx.T], axis=0)
    bx = np.concatenate([bx, bx], axis=0)
    return [jnp.asarray(m, BF16) for m in (forward, across, bx, adjoint, gather)]


def split(x):
    high = x.astype(BF16)
    return high, (x - high.astype(F32)).astype(BF16)


def dot(a, b):
    return jnp.dot(a, b, preferred_element_type=F32)


def field(coeffs, wf, bxt, out):
    high, low = split(coeffs)
    first = dot(wf, jnp.concatenate([high, high, low], axis=0))
    high, low = split(first)
    for c in range(3):
        cols = slice(c * 128, c * 128 + 128)
        out[c] = dot(jnp.concatenate([high[:, cols], low[:, cols]], axis=1), bxt) * SCALE


def send(src, dst, send_sem, recv_sem, **where):
    return pltpu.make_async_remote_copy(
        src_ref=src,
        dst_ref=dst,
        send_sem=send_sem,
        recv_sem=recv_sem,
        device_id=where,
        device_id_type=MESH,
    )


def by_groups(first, last, size, body):
    assert (last - first) % size == 0

    def group(i):
        for j in range(size):
            body(first + i * size + j)

    each(0, (last - first) // size, group)


def greet(barrier, **where):
    pl.semaphore_signal(barrier, inc=1, device_id=where, device_id_type=MESH)


def wait_in(ref, sem, **where):
    send(ref, ref, sem, sem, **where).wait_recv()


def wait_out(ref, sem, **where):
    send(ref, ref, sem, sem, **where).wait_send()


def each(first, last, body):
    def step(i, carry):
        body(i)
        return carry

    lax.fori_loop(first, last, step, 0)


def pick(shift, values):
    odd, top = shift
    steps = [jnp.where(odd, values[i + 1], values[i]) for i in range(4)]
    return jnp.where(top, steps[2], steps[0]), jnp.where(top, steps[3], steps[1])


def pick_many(shift, groups):
    pairs = [pick(shift, values) for values in zip(*groups)]
    return [p[0] for p in pairs], [p[1] for p in pairs]


def warp(lows, steps, u, current):
    th = [jnp.tanh(x) for x in u]
    fz, fy, fx = [0.5 + 0.5 * t for t in th]
    along = [low + fx * step for low, step in zip(lows, steps)]
    slope_y = [along[1] - along[0], along[3] - along[2]]
    along_y = [along[0] + fy * slope_y[0], along[2] + fy * slope_y[1]]
    slope_x = [steps[0] + fy * (steps[1] - steps[0]), steps[2] + fy * (steps[3] - steps[2])]
    slopes = [
        along_y[1] - along_y[0],
        slope_y[0] + fz * (slope_y[1] - slope_y[0]),
        slope_x[0] + fz * (slope_x[1] - slope_x[0]),
    ]
    warped = along_y[0] + fz * slopes[0]
    resid = warped - current
    return warped, [resid * slope * (1.0 - t * t) for slope, t in zip(slopes, th)]


def main_kernel(
    slabs, cohort, subject, offsets_in, template_in, control, wf_in, bxt_in, bx_in, wa_in, gather_in,
    mean_out, bulk_out, rest_out,
    own, peer, band, u0, offsets, template, wf, bxt, bx, wa, gather,
    shifted, corners, grad, warped, current, moved, terms, grid,
    small, piece, summed, pieces, means, wide, wide_means, peaks, mine, bulk, rest,
    in_sem, halo_sem, know_sem, know_subj_sem, ex_sem, pk_sem, rs_sem, tg_sem, ag_sem, fw_sem,
):
    me = lax.axis_index("slab")
    core = lax.axis_index("yslab")
    who = lax.axis_index("subj")
    other = 1 - core
    depth = offsets.shape[1]
    share = depth // cohort * 8
    far = slabs // 2
    hop = slabs // 4

    def slab_at(d):
        return lax.rem(me + (d + slabs), slabs)

    def subj_at(d):
        return lax.rem(who + (d + cohort), cohort)

    up, down = slab_at(1), slab_at(-1)
    barrier = pltpu.get_barrier_semaphore()
    greet(barrier, yslab=other)
    for slab in (up, down):
        greet(barrier, slab=slab)
        greet(barrier, slab=slab, yslab=other)
    for d in (1, -1):
        greet(barrier, subj=subj_at(d))

    rows_in = control.shape[0] // 3
    begin = jnp.minimum(me * (depth // KNOT * 7), rows_in - 56)
    late = jnp.where(me == slabs - 1, 1, 0)
    inner = pl.ds(HALO, depth)
    fetch_subject = pltpu.make_async_copy(subject, own.at[inner], in_sem.at[0])
    fetch_control = [
        pltpu.make_async_copy(
            control.at[pl.ds(c * rows_in + begin, 56), 0],
            band.at[pl.ds(0, 56), pl.ds(c * 128, 128)],
            in_sem.at[1 + c],
        )
        for c in range(3)
    ]
    fetch_rest = [
        pltpu.make_async_copy(src, dst, in_sem.at[4 + i])
        for i, (src, dst) in enumerate(
            [
                (wf_in.at[core, late], wf.at[0]),
                (bxt_in, bxt),
                (wf_in.at[core, 2], wf.at[1]),
                (offsets_in, offsets),
                (template_in, template),
                (bx_in, bx),
                (wa_in, wa),
                (gather_in, gather),
                (control.at[pl.ds(0, bulk.shape[0]), 0], bulk),
                (control.at[pl.ds(bulk.shape[0], rest.shape[0])], rest),
            ]
        )
    ]
    for copy in [fetch_subject] + fetch_control + fetch_rest:
        copy.start()
    band[56:64, :] = jnp.zeros((8, 384), F32)

    pl.semaphore_wait(barrier, 7)
    fetch_subject.wait()
    low = pl.ds(0, HALO)
    high = pl.ds(depth + HALO, HALO)
    first = pl.ds(HALO, HALO)
    last = pl.ds(depth, HALO)
    across = send(own.at[inner], peer.at[inner], halo_sem.at[0], halo_sem.at[1], yslab=other)
    along = [
        send(own.at[last], own.at[low], halo_sem.at[2], halo_sem.at[3], slab=up),
        send(own.at[first], own.at[high], halo_sem.at[2], halo_sem.at[3], slab=down),
        send(own.at[last], peer.at[low], halo_sem.at[2], halo_sem.at[3], slab=up, yslab=other),
        send(own.at[first], peer.at[high], halo_sem.at[2], halo_sem.at[3], slab=down, yslab=other),
    ]
    for copy in along + [across]:
        copy.start()

    know_slab = [1]
    know_subj = [1]

    def tell():
        if know_slab[0] < far:
            r = know_slab[0].bit_length() - 1
            for d in (know_slab[0], -know_slab[0]):
                greet(know_sem.at[r], slab=slab_at(d))
        if know_subj[0] < cohort // 2:
            r = know_subj[0].bit_length() - 1
            for d in (know_subj[0], -know_subj[0]):
                greet(know_subj_sem.at[r], subj=subj_at(d))

    def learn():
        if know_slab[0] < far:
            pl.semaphore_wait(know_sem.at[know_slab[0].bit_length() - 1], 2)
            know_slab[0] *= 2
        if know_subj[0] < cohort // 2:
            pl.semaphore_wait(know_subj_sem.at[know_subj[0].bit_length() - 1], 2)
            know_subj[0] *= 2

    tell()

    for copy in fetch_control + fetch_rest[:2]:
        copy.wait()
    field(band[...], wf[0], bxt[...], u0)

    lane = lax.broadcasted_iota(jnp.int32, (8, 128), 1)
    below = core.astype(F32)
    above = 1.0 - below

    def build(source, places, z):
        out_low = jnp.logical_and(z < HALO, me == 0)
        out_high = jnp.logical_and(z >= depth + HALO, me == slabs - 1)
        keep = jnp.where(jnp.logical_or(out_low, out_high), 0.0, 1.0)
        plane = source[z].astype(F32) * keep
        a, b = plane[:, :128], plane[:, 128:]
        for move in range(-HALO, HALO + 1):
            if move == 0:
                ra, rb = a, b
            else:
                ra = pltpu.roll(a, (-move) % 128, 1)
                rb = pltpu.roll(b, (-move) % 128, 1)
                if move < 0:
                    ra, rb = (
                        jnp.where(lane < -move, 0.0, ra),
                        jnp.where(lane < -move, ra, rb),
                    )
                else:
                    ra, rb = (
                        jnp.where(lane >= 128 - move, rb, ra),
                        jnp.where(lane >= 128 - move, 0.0, rb),
                    )
            for row, factor in places:
                for half, value in enumerate((ra, rb)):
                    if factor is not None:
                        value = value * factor
                    shifted[move + HALO, z, half, row : row + 8, :] = value

    at_own = ((8, None),)
    at_peer = ((0, below), (16, above))

    def edge_of(i, top):
        return jnp.where(i < HALO, i, i + (top - HALO))

    by_groups(HALO, depth + HALO, 4, lambda z: build(own, at_own, z))
    learn()
    tell()
    across.wait()
    by_groups(HALO, depth + HALO, 4, lambda z: build(peer, at_peer, z))
    for copy in fetch_rest[2:-2]:
        copy.wait()

    def first_warp(z):
        rows = pl.ds(pl.multiple_of(z * 8, 8), 8)
        for half in range(2):
            cols = pl.ds(half * 128, 128)
            shift = []
            for c in range(3):
                value = offsets[c, z, :, cols]
                shift.append(((value & 1) == 1, value >= 0))
            planes = []
            for mz in range(5):
                lines = []
                for my in range(5):
                    values = [shifted[mx, z + mz, half, 6 + my : 14 + my, :] for mx in range(5)]
                    lines.append(list(pick(shift[2], values)))
                low, high = pick_many(shift[1], lines)
                planes.append(low + high)
            low, high = pick_many(shift[0], planes)
            found = low + high
            lows = found[0::2]
            steps = [found[2 * i + 1] - found[2 * i] for i in range(4)]
            for i in range(4):
                corners[i, rows, cols] = lows[i]
                corners[4 + i, rows, cols] = steps[i]
            u = [u0[c, rows, cols] for c in range(3)]
            value, slopes = warp(lows, steps, u, template[rows, cols])
            warped[rows, cols] = value
            for c in range(3):
                grad[c, rows, cols] = slopes[c]

    each(HALO, depth - HALO, first_warp)
    learn()
    tell()
    planes = own.at[pl.ds(0, 4 * HALO)]
    wait_in(planes, halo_sem.at[3], slab=up)
    wait_out(planes, halo_sem.at[2], slab=up)

    def build_edge(i):
        z = edge_of(i, depth + HALO)
        build(own, at_own, z)
        build(peer, at_peer, z)

    by_groups(0, 2 * HALO, 2, build_edge)
    each(0, 2 * HALO, lambda i: first_warp(edge_of(i, depth - HALO)))
    while know_subj[0] < cohort // 2:
        learn()
        tell()

    def part_of(ref, p):
        return ref.at[pl.ds(pl.multiple_of(p * share, share), share)]

    def own_rows(ref):
        return ref[pl.ds(pl.multiple_of(who * share, share), share), :]

    others = [d for d in range(1, cohort)]

    def scatter(it, source, slots):
        for d in others:
            p = subj_at(d)
            send(part_of(source, p), slots.at[who], rs_sem.at[it, 0], rs_sem.at[it, 1], subj=p).start()

    def spread(it, source, slots):
        for d in others:
            send(source, slots.at[who], tg_sem.at[it, 0], tg_sem.at[it, 1], subj=subj_at(d)).start()

    def got(it, slots, sem):
        several = slots.at[pl.ds(0, cohort - 1)]
        wait_in(several, sem.at[it, 1], subj=subj_at(1))
        wait_out(several, sem.at[it, 0], subj=subj_at(1))

    def adjoint(it):
        firsts = []
        for c in range(3):
            high, low = split(grad[c])
            firsts.append(dot(jnp.concatenate([high, low], axis=1), bx[...]))
        high, low = split(jnp.concatenate(firsts, axis=1))
        part = dot(wa[...], jnp.concatenate([high, high, low], axis=0)) * SCALE
        for g in range(3):
            terms[it, 3 * core + g] = part[16 * g : 16 * g + 16].astype(BF16)

    def exchange(it):
        mine_rows = terms.at[it, pl.ds(3 * core, 3)]
        lower = terms.at[it, 3 * core]
        upper = terms.at[it, 3 * core + 1]
        sems = (ex_sem.at[it, 0], ex_sem.at[it, 1])
        send(upper, terms.at[it, 6 + core], *sems, slab=up, yslab=other).start()
        send(lower, terms.at[it, 8 + core], *sems, slab=down, yslab=other).start()
        send(upper, terms.at[it, 6 + core], *sems, slab=up).start()
        send(lower, terms.at[it, 8 + core], *sems, slab=down).start()
        send(mine_rows, mine_rows, *sems, yslab=other).start()

    def got_exchange(it):
        several = terms.at[it, pl.ds(0, 7)]
        wait_in(several, ex_sem.at[it, 1], yslab=other)
        wait_out(several, ex_sem.at[it, 0], yslab=other)

    def reduce_terms(it):
        edge = jnp.where(me == 0, 1, jnp.where(me == slabs - 1, 2, 0))
        total = dot(gather[edge], terms[it].reshape(160, 384))
        squares = total * total
        squares = squares[:, :128] + squares[:, 128:256] + squares[:, 256:]
        peak = jnp.sqrt(jnp.max(squares, axis=(0, 1), keepdims=True))
        mine[...] = jnp.broadcast_to(peak, (1, 128))
        p0 = peak.astype(BF16).astype(F32)
        p1 = (peak - p0).astype(BF16).astype(F32)
        p2 = peak - p0 - p1
        wide_peak = jnp.concatenate([jnp.broadcast_to(p, (64, 128)) for p in (p0, p1, p2)], axis=1)
        row = lax.broadcasted_iota(jnp.int32, (64, 384), 0)
        packed = jnp.where((row & 7) == 7, wide_peak, total).astype(BF16)
        grid[...] = total
        lowest = packed[0:16], packed[32:48]
        highest = packed[16:32], packed[48:64]
        pieces[it, core, me] = jnp.where(core == 0, lowest[0], highest[0])

        @pl.when(me == slabs - 1)
        def _():
            pieces[it, core, slabs] = jnp.where(core == 0, lowest[1], highest[1])

    def send_peaks():
        peaks[me] = mine[...]
        for i in range(slabs - 1):
            d = far if i == 0 else (far - (i + 1) // 2) * (1 if i % 2 else -1)
            send(mine, peaks.at[me], pk_sem.at[0], pk_sem.at[1], slab=slab_at(d)).start()

    def got_peaks():
        several = peaks.at[pl.ds(0, slabs - 1)]
        wait_in(several, pk_sem.at[1], slab=up)
        wait_out(several, pk_sem.at[0], slab=up)
        return STEP / (jnp.max(peaks[...], axis=0) + TINY)

    end = slabs - 1

    def blocks(it, origin, count):
        return pieces.at[it, core, pl.ds(origin, count)]

    def ship(it, origin, sent, targets):
        for ends, count in ((origin == end, 2), (origin != end, 1)):

            @pl.when(ends)
            def _():
                ref = blocks(it, origin, count)
                for d, place in targets:
                    send(ref, ref, ag_sem.at[it, sent], ag_sem.at[it, place], slab=slab_at(d)).start()

    def settle(it, count, extra, origins, wait, place):
        found = origins[0] == end
        for origin in origins[1:]:
            found = jnp.logical_or(found, origin == end)
        for case, number in ((found, count + extra), (jnp.logical_not(found), count)):

            @pl.when(case)
            def _():
                wait(blocks(it, 0, number), ag_sem.at[it, place], slab=up)

    OWN, EDGE_UP, EDGE_DOWN, NEAR, FAR, GO_UP, GO_DOWN = range(7)

    def send_edges(it):
        ship(it, me, OWN, [(hop, EDGE_UP), (-hop, EDGE_DOWN)])

    def send_near(it):
        targets = []
        for d in range(hop - 1, 0, -1):
            targets += [(d, NEAR), (-d, NEAR)]
        if targets:
            ship(it, me, OWN, targets)

    def hand_on(it):
        origin = slab_at(-hop)
        settle(it, 1, 1, [origin], wait_in, EDGE_UP)
        ship(it, origin, GO_UP, [(d, FAR) for d in range(hop, 0, -1)])
        origin = slab_at(hop)
        settle(it, 1, 1, [origin], wait_in, EDGE_DOWN)
        ship(it, origin, GO_DOWN, [(-d, FAR) for d in range(hop - 1, 0, -1)])

    def got_grid(it):
        near = [slab_at(d) for d in range(1 - hop, hop) if d != 0]
        if near:
            settle(it, len(near), 1, near, wait_in, NEAR)
        distant = [slab_at(d) for d in range(hop + 1, slabs - hop)]
        settle(it, len(distant), 1, distant, wait_in, FAR)
        both = pieces.at[it, core]
        send(both, both, fw_sem.at[it, 0], fw_sem.at[it, 1], yslab=other).start()

    def sent_grid(it):
        both = pieces.at[it, core]
        send(both, both, fw_sem.at[it, 0], fw_sem.at[it, 1], yslab=other).wait()
        for origin, count, sent in (
            (me, 2 * hop, OWN),
            (slab_at(-hop), hop, GO_UP),
            (slab_at(hop), hop - 1, GO_DOWN),
        ):
            if count:
                settle(it, count, count, [origin], wait_out, sent)

    small[...] = warped[...].astype(BF16)
    piece[who] = own_rows(small)
    scatter(0, small, piece)
    adjoint(0)
    exchange(0)
    while know_slab[0] < far:
        learn()
        tell()
    got_exchange(0)
    reduce_terms(0)
    send_peaks()
    send_edges(0)
    got(0, piece, rs_sem)
    total = piece[0].astype(F32)
    for p in range(1, cohort):
        total = total + piece[p].astype(F32)
    summed[...] = (total / cohort).astype(BF16)
    means[who] = summed[...]
    spread(0, summed, means)
    field(grid[...], wf[1], bxt[...], moved)
    send_near(0)
    hand_on(0)
    factor_1 = got_peaks()
    got(0, means, tg_sem)
    for p in range(cohort):
        current[p * share : p * share + share] = means[p].astype(F32)

    def second_warp(z):
        rows = pl.ds(pl.multiple_of(z * 8, 8), 8)
        for half in range(2):
            cols = pl.ds(half * 128, 128)
            lows = [corners[i, rows, cols] for i in range(4)]
            steps = [corners[4 + i, rows, cols] for i in range(4)]
            u = [u0[c, rows, cols] - factor_1 * moved[c, rows, cols] for c in range(3)]
            value, slopes = warp(lows, steps, u, current[rows, cols])
            warped[rows, cols] = value
            for c in range(3):
                grad[c, rows, cols] = slopes[c]

    by_groups(0, depth, 2, second_warp)
    wide[who] = own_rows(warped)
    adjoint(1)
    exchange(1)
    scatter(1, warped, wide)
    got_exchange(1)
    reduce_terms(1)
    send_edges(1)
    got_grid(0)
    got(1, wide, rs_sem)
    total = wide[0]
    for p in range(1, cohort):
        total = total + wide[p]
    total = total / cohort
    current[0:share] = total
    wide_means[who] = total
    spread(1, current.at[pl.ds(0, share)], wide_means)
    send_near(1)
    hand_on(1)
    sent_grid(0)
    got_grid(1)
    got(1, wide_means, tg_sem)
    for p in range(cohort):
        mean_out[p * share : p * share + share] = wide_means[p]
    sent_grid(1)

    peak = None
    for k in range(2):
        for slab in range(slabs):
            row = pieces[1, k, slab, 7:8, :].astype(F32)
            row = (row[:, :128] + row[:, 128:256]) + row[:, 256:]
            peak = row if peak is None else jnp.maximum(peak, row)
    factor_2 = STEP / (peak + TINY)
    for copy in fetch_rest[-2:]:
        copy.wait()
    grid_rows = control.shape[0] // 21
    sub = lax.broadcasted_iota(jnp.int32, (8, 128), 0)
    made = {}

    def change(s):
        if s not in made:
            c, a = divmod(s, grid_rows)
            cols = slice(c * 128, c * 128 + 128)
            k, slab, i = (a // 2) % 2, a // 4, a % 2
            one, two = (
                pieces[it, k, slab, :, cols].astype(F32)[8 * i : 8 * i + 8] for it in range(2)
            )
            made[s] = factor_1 * one + factor_2 * two
        return made[s]

    for t in range((3 * grid_rows * 7 + 7) // 8):
        s, skip = divmod(8 * t, 7)
        value = change(s)
        if skip:
            value = pltpu.roll(value, 8 - skip, 0)
        if s + 1 < 3 * grid_rows:
            after = pltpu.roll(change(s + 1), 7 - skip, 0)
            value = jnp.where(sub < 7 - skip, value, after)
            rows = pl.ds(8 * t, 8)
            bulk_out[rows, :] = bulk[rows, :] - value
        else:
            for j in range(rest.shape[0]):
                rest_out[j] = rest[j] - value[j : j + 1]
        made.pop(s - 1, None)


def write_kernel(mean, bulk, rest, mean_out, control_out, sems):
    copies = [
        pltpu.make_async_copy(bulk, control_out.at[pl.ds(0, bulk.shape[0]), 0], sems.at[0]),
        pltpu.make_async_copy(
            rest, control_out.at[pl.ds(bulk.shape[0], rest.shape[0])], sems.at[1]
        ),
        pltpu.make_async_copy(mean, mean_out, sems.at[2]),
    ]
    for copy in copies:
        copy.start()
    for copy in copies:
        copy.wait()


def solution(mesh):
    slabs = mesh.shape["slab"]
    cohort = mesh.shape["subj"]
    assert mesh.shape["yslab"] == 2 and slabs >= 4 and slabs % 4 == 0

    def shards(subjects, offsets, template, control):
        depth, height, width = subjects.shape[1:]
        rows = depth * height
        share = rows // cohort
        wf, bxt, bx, wa, gather = constants(depth, height, width, control.shape[4])
        vmem = pltpu.VMEM
        dma = pltpu.SemaphoreType.DMA
        plain = pltpu.SemaphoreType.REGULAR
        deep = depth + 2 * HALO
        grid_rows = control.shape[2]
        rounds = (slabs // 2).bit_length() - 1
        dense = control.reshape(3 * grid_rows * 7, 1, 128)
        left = dense.shape[0] % 8
        assert left
        args = (
            subjects[0],
            offsets[0],
            template.reshape(rows, width),
            dense,
            wf, bxt, bx, wa, gather,
        )
        mean, bulk, rest = pl.pallas_call(
            lambda *refs: main_kernel(slabs, cohort, *refs),
            out_shape=[
                jax.ShapeDtypeStruct((rows, width), F32),
                jax.ShapeDtypeStruct((dense.shape[0] - left, 128), F32),
                jax.ShapeDtypeStruct((left, 1, 128), F32),
            ],
            in_specs=[pl.BlockSpec(memory_space=pltpu.HBM)] * len(args),
            out_specs=[pl.BlockSpec(memory_space=vmem)] * 3,
            scratch_shapes=[
                vmem((deep, height, width), BF16),
                vmem((deep, height, width), BF16),
                vmem((64, 384), F32),
                vmem((3, rows, width), F32),
                vmem((3, depth, height, width), jnp.int32),
                vmem((rows, width), F32),
                vmem((2, *wf.shape[2:]), BF16),
                vmem(bxt.shape, BF16),
                vmem(bx.shape, BF16),
                vmem(wa.shape, BF16),
                vmem(gather.shape, BF16),
                vmem((5, deep, 2, 24, 128), F32),
                vmem((8, rows, width), F32),
                vmem((3, rows, width), F32),
                vmem((rows, width), F32),
                vmem((rows, width), F32),
                vmem((3, rows, width), F32),
                vmem((2, 10, 16, 384), BF16),
                vmem((64, 384), F32),
                vmem((rows, width), BF16),
                vmem((cohort, share, width), BF16),
                vmem((share, width), BF16),
                vmem((2, 2, slabs + 1, 16, 384), BF16),
                vmem((cohort, share, width), BF16),
                vmem((cohort, share, width), F32),
                vmem((cohort, share, width), F32),
                vmem((slabs, 1, 128), F32),
                vmem((1, 128), F32),
                vmem((dense.shape[0] - left, 128), F32),
                vmem((left, 1, 128), F32),
                dma((14,)),
                dma((4,)),
                plain((rounds,)),
                plain((max((cohort // 2).bit_length() - 1, 1),)),
                dma((2, 2)),
                dma((2,)),
                dma((2, 2)),
                dma((2, 2)),
                dma((2, 7)),
                dma((2, 2)),
            ],
            compiler_params=pltpu.CompilerParams(
                collective_id=0, has_side_effects=True, vmem_limit_bytes=48 * 1024 * 1024
            ),
            name="register",
        )(*[pltpu.with_memory_space_constraint(a, pltpu.HBM) for a in args])
        mean, dense = pl.pallas_call(
            write_kernel,
            out_shape=[
                jax.ShapeDtypeStruct((rows, width), F32),
                jax.ShapeDtypeStruct(dense.shape, F32),
            ],
            in_specs=[pl.BlockSpec(memory_space=vmem)] * 3,
            out_specs=[pl.BlockSpec(memory_space=pltpu.HBM)] * 2,
            scratch_shapes=[dma((3,))],
            compiler_params=pltpu.CompilerParams(vmem_limit_bytes=4 * 1024 * 1024),
            name="write",
        )(mean, bulk, rest)
        return mean.reshape(depth, height, width), dense.reshape(control.shape)

    in_specs = (
        P(("group", "subj"), "slab", "yslab", None),
        P(("group", "subj"), None, "slab", "yslab", None),
        P(("group", "slab"), "yslab", None),
        P(("group", "subj"), None, None, None, None),
    )
    out_specs = (P(("group", "slab"), "yslab", None), P(("group", "subj"), None, None, None, None))
    return jax.shard_map(shards, mesh=mesh, in_specs=in_specs, out_specs=out_specs, check_vma=False)
```
